32 devices in a mesh: dp: 4 (over y, x), row: 2 (over core), col: 4 (over z).
Axes of the slice: x: 2, y: 2, z: 4, core: 2. Of those that a mesh axis runs over, the one named last changes fastest.
Arguments:
- x_in: bfloat16 [4096, 2048], P(('dp', 'col'), 'row'), may hold values from -6 to 6
- cotangent: bfloat16 [4096, 2048], P(('dp', 'col'), 'row'), may hold values from -6 to 6
- segment_ids: int32 [4, 1024], P('dp'), may hold values from 0 to 7, never falling along the last dimension, each value on 1 to 512 neighbouring positions
- owner: int32 [4], replicated, may hold values from 0 to 3, as said below
- w_mix_in: bfloat16 [2048, 8240], P('row', 'col'), may hold values from -0.125 to 0.125
- w_mix_out: bfloat16 [4096, 2048], P('col', 'row'), may hold values from -0.1875 to 0.1875
- w_gate_up: bfloat16 [2048, 8192], P('row', 'col'), may hold values from -0.125 to 0.125
- w_down: bfloat16 [4096, 2048], P('col', 'row'), may hold values from -0.09375 to 0.09375
- mat_m: float32 [2, 4, 4, 4218880], P('row', 'col', 'dp'), as said below
- mat_v: float32 [2, 4, 4, 4218880], P('row', 'col', 'dp'), as said below
- small_params: float32 [22160], replicated, as said below
- small_m: float32 [22160], replicated, may hold values from -128 to 128
- small_v: float32 [22160], replicated, may hold values from 100 to 10000
Outputs:
- y_out: bfloat16 [4096, 2048], P(('dp', 'col'), 'row')
- x_grad: bfloat16 [4096, 2048], P(('dp', 'col'), 'row')
- mat_grad: float32 [2, 4, 4, 4218880], P('row', 'col', 'dp')
- mat_m_new: float32 [2, 4, 4, 4218880], P('row', 'col', 'dp')
- mat_v_new: float32 [2, 4, 4, 4218880], P('row', 'col', 'dp')
- mat_update: float32 [2, 4, 4, 4218880], P('row', 'col', 'dp')
- new_mix_in: bfloat16 [2048, 8240], P('row', 'col')
- new_mix_out: bfloat16 [4096, 2048], P('col', 'row')
- new_gate_up: bfloat16 [2048, 8192], P('row', 'col')
- new_down: bfloat16 [4096, 2048], P('col', 'row')
- small_grad: float32 [22160], replicated
- small_m_new: float32 [22160], replicated
- small_v_new: float32 [22160], replicated
- small_update: float32 [22160], replicated
The draws below stay inside these ranges and needn't reach their ends.
Inputs may be any that keep to these rules, and one draw needn't show every extreme that they name: owner[i] is an owner group; one group owns exactly 2 matrices, every other group at most one. `mat_m`: each matrix's block lies in its owner group's buffer as stated in the reference program; all other entries are zero. `mat_v`: positive on the entries of owned blocks, zero elsewhere. `small_params`: gains near one, skip terms positive, convolution terms of any sign.
All inputs are finite; a program needn't handle non-finite values.
Results may differ from the reference program's by a relative error of at most 0.03.
Values may be sent and summed in bfloat16 or wider, within the bound.
A program may use at most 320 MiB of HBM per device.

```python
import math
import jax
import jax.numpy as jnp
import numpy as np
from jax import lax

D = 2048
FF = 4096
QH = 8
KVH = 2
HD = 128
SH = 48
SP = 64
STATE = 256
CONV = 4
SPAN = 128
SEQ = 1024
DOCS = 8
MATS = 4
OWNERS = 4
SLOTS = 2
STEP = 4
TOKENS = 4096
DR = 1024
QC = 256
SC = 256
EC = 768
FC = 1024
CI = 2060
MO = 1024
MIXW = 8240
CH = 3584
SMALL = 22160
SLOT = 2109440
CAP = 4218880
PIECE = 4218880
N_DP = 4
N_ROW = 2
N_COL = 4


def owner_table(key):
    groups = jax.random.permutation(jax.random.fold_in(key, 11), OWNERS).astype(jnp.int32)
    order = jax.random.permutation(jax.random.fold_in(key, 13), MATS).astype(jnp.int32)
    light_index = 1 + jnp.maximum(order - SLOTS, 0) % (OWNERS - 1)
    return jnp.where(order < SLOTS, groups[0], groups[light_index]).astype(jnp.int32)


def used_cells(key):
    owners = owner_table(key)
    block_sizes = [DR * CI, MO * DR, DR * 2 * FC, FC * DR]
    group = jnp.arange(OWNERS)[:, None]
    position = jnp.arange(CAP)[None, :]
    marked = jnp.zeros((OWNERS, CAP), jnp.float32)
    for matrix_index in range(MATS):
        earlier = jnp.int32(0)
        for earlier_index in range(matrix_index):
            earlier = earlier + (owners[earlier_index] == owners[matrix_index]).astype(jnp.int32)
        offset = earlier * SLOT
        inside = (group == owners[matrix_index]) & (position >= offset) & (position < offset + block_sizes[matrix_index])
        marked = jnp.where(inside, 1.0, marked)
    return marked.reshape(N_DP, PIECE)


def draw_owner(key, part):
    return owner_table(key)


def draw_mat_m(key, part):
    values = jax.random.normal(jax.random.fold_in(key, 23), (N_ROW, N_COL, N_DP, PIECE), jnp.float32) * 30.0
    return values * used_cells(key)[None, None]


def draw_mat_v(key, part):
    spread = jax.random.uniform(jax.random.fold_in(key, 29), (N_ROW, N_COL, N_DP, PIECE), jnp.float32, math.log(300.0), math.log(3000.0))
    return jnp.exp(spread) * used_cells(key)[None, None]


def draw_small_params(key, part):
    subkeys = jax.random.split(jax.random.fold_in(key, 37), 6)
    gains = 1.0 + 0.1 * jax.random.uniform(subkeys[0], (2 * D,), jnp.float32, -2.0, 2.0)
    log_rates = jax.random.uniform(subkeys[1], (SH,), jnp.float32, math.log(0.03), math.log(1.5))
    step_bias = jax.random.uniform(subkeys[2], (SH,), jnp.float32, -5.0, -3.0)
    skips = jax.random.uniform(subkeys[3], (SH,), jnp.float32, 0.5, 1.5)
    kernel = jax.random.normal(subkeys[4], (CONV * CH,), jnp.float32) * 0.5
    conv_bias = jax.random.normal(subkeys[5], (CH,), jnp.float32) * 0.2
    return jnp.concatenate([gains, log_rates, step_bias, skips, kernel, conv_bias], 0)


def block_scale(rng, dims, cuts, smallest, top_value):
    loudness, own = 1.0, jax.random.fold_in(rng, 6)
    for dim, shards_of in cuts:
        heights = jnp.exp(jax.random.uniform(jax.random.fold_in(own, dim), (shards_of,), jnp.float32, smallest / len(cuts), top_value / len(cuts)))
        loudness = loudness * jnp.repeat(heights, dims[dim] // shards_of).reshape([-1 if axis == dim else 1 for axis in range(len(dims))])
    return loudness


def split_up(amount, total, reach, skew):
    portions = [(1 << 20) // math.isqrt(grade ** skew) + 1 for grade in range(2, amount + 1)]
    surplus, holding = total - reach - (amount - 1), [1] * (amount - 1)
    while surplus > 0:
        candidates = [i for i in range(amount - 1) if holding[i] < reach]
        pool, left = sum([portions[i] for i in candidates]), surplus
        for i in candidates:
            extra = min(reach - holding[i], max(1, left * portions[i] // pool), surplus)
            holding[i] = holding[i] + extra
            surplus = surplus - extra
    return np.array([reach] + holding)


def uneven_parts(rng, number_of, total, reach, skew):
    if number_of == 2:
        one = jax.random.randint(rng, (), max(1, total - reach), min(reach, total - 1) + 1)
        return jnp.stack([one, total - one])
    tallies = jnp.asarray(split_up(number_of, total, reach, skew), jnp.int32)
    pairs = (number_of - 1) // 2
    giver, sink = tallies[1:1 + 2 * pairs:2], tallies[2:2 + 2 * pairs:2]
    slack = jnp.minimum(giver - 1, reach - sink)
    passed = jax.random.randint(jax.random.fold_in(rng, 1), (pairs,), 0, 1 << 20) % (slack + 1)
    tallies = tallies.at[1:1 + 2 * pairs:2].set(giver - passed).at[2:2 + 2 * pairs:2].set(sink + passed)
    return tallies[jax.random.permutation(jax.random.fold_in(rng, 2), number_of)]


def gaussian(key, dims, width, reach, pieces=(), held_as=jnp.bfloat16):
    loudness = block_scale(key, dims, pieces, -0.22, 0.18) if pieces else 1.0
    entries = jax.random.normal(key, dims, jnp.float32) * width * loudness
    return jnp.minimum(jnp.maximum(entries, -reach), reach).astype(held_as)


def setup_inputs(seed: int = 0) -> dict:
    key_of = jax.random.split(jax.random.key(seed), 14)
    return {
        "x_in": gaussian(key_of[0], (TOKENS, D), 1.0, 6.0, ((0, 16), (1, 2))),
        "cotangent": gaussian(key_of[1], (TOKENS, D), 1.0, 6.0, ((0, 16), (1, 2))),
        "segment_ids": jax.vmap(lambda own: jnp.searchsorted(jnp.cumsum(uneven_parts(own, DOCS, SEQ, SEQ // 2, 2)), jnp.arange(SEQ), side="right"))(jax.random.split(key_of[2], N_DP)).reshape((N_DP, SEQ)).astype(jnp.int32),
        "owner": draw_owner(jax.random.fold_in(key_of[13], 71), 0),
        "w_mix_in": gaussian(key_of[4], (D, MIXW), D ** -0.5, 0.125, ((0, 2), (1, 4))),
        "w_mix_out": gaussian(key_of[5], (MO * N_COL, D), 1024 ** -0.5, 0.1875, ((0, 4), (1, 2))),
        "w_gate_up": gaussian(key_of[6], (D, 2 * FF), D ** -0.5, 0.125, ((0, 2), (1, 4))),
        "w_down": gaussian(key_of[7], (FF, D), FF ** -0.5, 0.09375, ((0, 4), (1, 2))),
        "mat_m": draw_mat_m(jax.random.fold_in(key_of[13], 71), 0),
        "mat_v": draw_mat_v(jax.random.fold_in(key_of[13], 71), 0),
        "small_params": draw_small_params(jax.random.fold_in(key_of[13], 71), 0),
        "small_m": gaussian(key_of[11], (SMALL,), 20.0, 128.0, (), jnp.float32),
        "small_v": jnp.clip(jnp.exp(jax.random.uniform(key_of[12], (SMALL,), jnp.float32, math.log(100.0), math.log(10000.0))), 100.0, 10000.0),
    }


@jax.custom_vjp
def low(v):
    return lax.optimization_barrier(v.astype(jnp.bfloat16)).astype(jnp.float32)

@jax.custom_vjp
def low_back(v):
    return v

def low_keep(v):
    return (low(v), None)

def low_pass(kept, grad):
    return (grad,)

def back_keep(v):
    return (v, None)

def back_low(kept, grad):
    return (low(grad),)
low.defvjp(low_keep, low_pass)
low_back.defvjp(back_keep, back_low)
highest = lax.Precision.HIGHEST
norm_eps = 1e-05
beta_one = 0.5
beta_two = 0.6
learn_rate = 0.02
adam_eps = 1e-08
weight_decay = 0.1
masked_score = -1e+30

def silu_value(values):
    return values * jax.nn.sigmoid(values)

def rms_norm(values, gain):
    return values * lax.rsqrt(lax.optimization_barrier(jnp.mean(values * values, axis=-1, keepdims=True)) + norm_eps) * gain

def causal_conv(values, kernel, conv_bias, segments):
    length = values.shape[0]
    summed = values * kernel[0]
    for lag_steps in range(1, CONV):
        shifted = jnp.concatenate([jnp.zeros((lag_steps, values.shape[1]), jnp.float32), values[:length - lag_steps]], 0)
        earlier_seg = jnp.concatenate([jnp.full((lag_steps,), -1, jnp.int32), segments[:length - lag_steps]], 0)
        keep_mask = (earlier_seg == segments).astype(jnp.float32)
        summed = summed + kernel[lag_steps] * shifted * keep_mask[:, None]
    return summed + conv_bias

def scan_blocks(x_three, b_float, c_float, step_sizes, rate, segments, prev_seg, start_state):
    token_count = x_three.shape[0]
    block_count = token_count // SPAN

    def one_block(running_carry, inputs):
        state_now, last_seg = running_carry
        x_block, b_block, c_block, dt_block, seg_block = inputs
        log_decay = dt_block * rate
        running = jnp.cumsum(log_decay, axis=0)
        positions = jnp.arange(SPAN)
        live_pairs = (seg_block[:, None] == seg_block[None, :]) & (positions[:, None] >= positions[None, :])
        decay_logs = running[:, None, :] - running[None, :, :]
        decay_table = jnp.where(live_pairs[:, :, None], jnp.exp(jnp.where(live_pairs[:, :, None], decay_logs, 0.0)), 0.0)
        intersection = jnp.dot(c_block, b_block.T, precision=highest)
        inflow = dt_block[:, :, None] * x_block
        output = jnp.einsum('tsh,shp->thp', decay_table * intersection[:, :, None], inflow, precision=highest)
        carried = jnp.exp(running) * (seg_block == last_seg).astype(jnp.float32)[:, None]
        output = output + carried[:, :, None] * jnp.einsum('hpn,tn->thp', state_now, c_block, precision=highest)
        tail_decay = jnp.exp(running[-1][None, :] - running) * (seg_block == seg_block[-1]).astype(jnp.float32)[:, None]
        fresh_state = jnp.einsum('sh,shp,sn->hpn', tail_decay, inflow, b_block, precision=highest)
        passing = jnp.exp(running[-1]) * (seg_block[-1] == last_seg).astype(jnp.float32)
        return ((passing[:, None, None] * state_now + fresh_state, seg_block[-1]), output)
    inputs = (x_three.reshape(block_count, SPAN, x_three.shape[1], x_three.shape[2]), b_float.reshape(block_count, SPAN, b_float.shape[1]), c_float.reshape(block_count, SPAN, c_float.shape[1]), step_sizes.reshape(block_count, SPAN, step_sizes.shape[1]), segments.reshape(block_count, SPAN))
    (state_end, last_seg), outputs = lax.scan(jax.checkpoint(one_block), (start_state, prev_seg), inputs)
    return (outputs.reshape(x_three.shape), state_end)

def attention(queries, keys, values, segments):
    group_size = QH // KVH
    block_rows = min(512, SEQ)
    block_count = SEQ // block_rows
    key_heads = keys.reshape(SEQ, KVH, HD)
    value_heads = values.reshape(SEQ, KVH, HD)
    positions = jnp.arange(SEQ).astype(jnp.int32)
    query_blocks = queries.reshape(block_count, block_rows, KVH, group_size, HD)
    starts = (jnp.arange(block_count) * block_rows).astype(jnp.int32)

    def one_block(inputs):
        query_block, first_row = inputs
        scores = jnp.einsum('qkgd,skd->kgqs', query_block, key_heads, precision=highest) * HD ** (-0.5)
        scores = low_back(scores)
        query_pos = first_row + jnp.arange(block_rows).astype(jnp.int32)
        query_seg = lax.dynamic_slice_in_dim(segments, first_row, block_rows)
        allowed = (positions[None, :] <= query_pos[:, None]) & (segments[None, :] == query_seg[:, None])
        scores = jnp.where(allowed, scores, masked_score)
        attn_probs = low(jax.nn.softmax(scores, axis=-1))
        return jnp.einsum('kgqs,skd->qkgd', attn_probs, value_heads, precision=highest).reshape(block_rows, QH * HD)
    outputs = lax.map(jax.checkpoint(one_block), (query_blocks, starts))
    return outputs.reshape(SEQ, QH * HD)

def one_sequence(hidden_in, segments, mix_in_w, mix_out_w, gate_up_w, down_w, small_w):
    gain_one = small_w[:D]
    gain_two = small_w[D:2 * D]
    a_log = small_w[2 * D:2 * D + SH]
    dt_bias = small_w[2 * D + SH:2 * D + 2 * SH]
    d_skip = small_w[2 * D + 2 * SH:2 * D + 3 * SH]
    kern_start = 2 * D + 3 * SH
    kernel = small_w[kern_start:kern_start + CONV * CH].reshape(CONV, CH)
    conv_bias = small_w[kern_start + CONV * CH:kern_start + (CONV + 1) * CH]
    act_one = low(rms_norm(hidden_in, gain_one))
    projected = low_back(jnp.dot(act_one, mix_in_w, precision=highest)).reshape(SEQ, N_COL, CI)
    queries = low(projected[:, :, :QC].reshape(SEQ, QH * HD))
    shared = projected[:, :, QC:QC + SC].reshape(SEQ, N_COL, 4, SC // 4)
    keys = low(shared[:, :, 0].reshape(SEQ, KVH * HD))
    values = low(shared[:, :, 1].reshape(SEQ, KVH * HD))
    b_in = shared[:, :, 2].reshape(SEQ, STATE)
    c_in = shared[:, :, 3].reshape(SEQ, STATE)
    z_gate = projected[:, :, QC + SC:QC + SC + EC].reshape(SEQ, SH * SP)
    x_pre = projected[:, :, QC + SC + EC:QC + SC + 2 * EC].reshape(SEQ, SH * SP)
    dt_proj = projected[:, :, QC + SC + 2 * EC:].reshape(SEQ, SH)
    conv_out = low_back(causal_conv(jnp.concatenate([x_pre, b_in, c_in], 1), kernel, conv_bias, segments))
    x_sig = low(silu_value(conv_out[:, :SH * SP]))
    b_sig = low(silu_value(conv_out[:, SH * SP:SH * SP + STATE]))
    c_sig = low(silu_value(conv_out[:, SH * SP + STATE:]))
    attended = attention(queries, keys, values, segments)
    step_sizes = jax.nn.softplus(dt_proj + dt_bias)
    rate = -jnp.exp(a_log)
    x_three = x_sig.reshape(SEQ, SH, SP)
    start_state = jnp.zeros((SH, SP, STATE), jnp.float32)
    y_ssm, state_end = scan_blocks(x_three, b_sig, c_sig, step_sizes, rate, segments, jnp.int32(-1), start_state)
    y_ssm = y_ssm + d_skip[None, :, None] * x_three
    gated = y_ssm.reshape(SEQ, SH * SP) * silu_value(z_gate)
    mix = jnp.concatenate([attended.reshape(SEQ, N_COL, QC), gated.reshape(SEQ, N_COL, EC)], 2).reshape(SEQ, N_COL * MO)
    mix = low_back(low(mix))
    hidden_one = hidden_in + low_back(jnp.dot(mix, mix_out_w, precision=highest))
    act_two = low(rms_norm(hidden_one, gain_two))
    gate_up = low_back(jnp.dot(act_two, gate_up_w, precision=highest)).reshape(SEQ, N_COL, 2 * FC)
    inner = low(silu_value(gate_up[:, :, :FC]) * gate_up[:, :, FC:]).reshape(SEQ, FF)
    return hidden_one + low_back(jnp.dot(inner, down_w, precision=highest))

def adam_step(gradient, moment, second, weight):
    moment_new = beta_one * moment + (1.0 - beta_one) * gradient
    second_new = beta_two * second + (1.0 - beta_two) * gradient * gradient
    first_hat = moment_new / (1.0 - beta_one ** STEP)
    second_hat = second_new / (1.0 - beta_two ** STEP)
    update = -learn_rate * (first_hat / (jnp.sqrt(second_hat) + adam_eps) + weight_decay * weight)
    return (moment_new, second_new, update)

def to_blocks(matrix, row_major, rows_blk, cols_blk):
    if row_major:
        return matrix.reshape(N_ROW, rows_blk, N_COL, cols_blk).transpose(0, 2, 1, 3).reshape(N_ROW, N_COL, rows_blk * cols_blk)
    return matrix.reshape(N_COL, rows_blk, N_ROW, cols_blk).transpose(2, 0, 1, 3).reshape(N_ROW, N_COL, rows_blk * cols_blk)

def from_blocks(blocks, row_major, rows_blk, cols_blk):
    table = blocks.reshape(N_ROW, N_COL, rows_blk, cols_blk)
    if row_major:
        return table.transpose(0, 2, 1, 3).reshape(N_ROW * rows_blk, N_COL * cols_blk)
    return table.transpose(1, 2, 0, 3).reshape(N_COL * rows_blk, N_ROW * cols_blk)

def reference(x_in, cotangent, segment_ids, owner, w_mix_in, w_mix_out, w_gate_up, w_down, mat_m, mat_v, small_params, small_m, small_v):
    inputs_float = x_in.astype(jnp.float32).reshape(N_DP, SEQ, D)
    weights = (w_mix_in.astype(jnp.float32), w_mix_out.astype(jnp.float32), w_gate_up.astype(jnp.float32), w_down.astype(jnp.float32))

    def forward(hidden_in, mix_in_w, mix_out_w, gate_up_w, down_w, small_w):

        def per_sequence(seq_pair):
            return one_sequence(seq_pair[0], seq_pair[1], mix_in_w, mix_out_w, gate_up_w, down_w, small_w)
        return lax.map(per_sequence, (hidden_in, segment_ids))
    layer_out, pullback = jax.vjp(forward, inputs_float, weights[0], weights[1], weights[2], weights[3], small_params)
    gradients = pullback(cotangent.astype(jnp.float32).reshape(N_DP, SEQ, D))
    layouts = ((True, DR, CI), (False, MO, DR), (True, DR, 2 * FC), (False, FC, DR))
    zero_index = jnp.int32(0)
    offsets = []
    for matrix_index in range(MATS):
        earlier = jnp.int32(0)
        for other_index in range(matrix_index):
            earlier = earlier + (owner[other_index] == owner[matrix_index]).astype(jnp.int32)
        offsets.append((earlier * SLOT).astype(jnp.int32))

    def place_all(matrices):
        buffer = jnp.zeros((N_ROW, N_COL, OWNERS, CAP), jnp.float32)
        for matrix_index in range(MATS):
            row_major, rows_blk, cols_blk = layouts[matrix_index]
            blocks = to_blocks(matrices[matrix_index], row_major, rows_blk, cols_blk)
            buffer = lax.dynamic_update_slice(buffer, blocks[:, :, None, :], (zero_index, zero_index, owner[matrix_index], offsets[matrix_index]))
        return buffer
    grad_buffer = place_all(gradients[1:5])
    weight_buffer = place_all(weights)
    group_shape = (N_ROW, N_COL, OWNERS, CAP)
    piece_shape = (N_ROW, N_COL, N_DP, PIECE)
    moment_new, second_new, update = adam_step(grad_buffer, mat_m.reshape(group_shape), mat_v.reshape(group_shape), weight_buffer)
    new_weights = []
    for matrix_index in range(MATS):
        row_major, rows_blk, cols_blk = layouts[matrix_index]
        block_update = lax.dynamic_slice(update, (zero_index, zero_index, owner[matrix_index], offsets[matrix_index]), (N_ROW, N_COL, 1, rows_blk * cols_blk))[:, :, 0]
        whole_update = from_blocks(block_update, row_major, rows_blk, cols_blk)
        new_weights.append((weights[matrix_index] + whole_update).astype(jnp.bfloat16))
    small_moment, small_second, small_update = adam_step(gradients[5], small_m, small_v, small_params)
    return (layer_out.reshape(TOKENS, D).astype(jnp.bfloat16), gradients[0].reshape(TOKENS, D).astype(jnp.bfloat16), grad_buffer.reshape(piece_shape), moment_new.reshape(piece_shape), second_new.reshape(piece_shape), update.reshape(piece_shape), new_weights[0], new_weights[1], new_weights[2], new_weights[3], gradients[5], small_moment, small_second, small_update)
```

```python
import functools

import jax
import jax.numpy as jnp
from jax import lax
from jax.experimental import pallas as pl
from jax.experimental.pallas import tpu as pltpu
from jax.sharding import PartitionSpec as P

D = 2048
FF = 4096
QH = 8
KVH = 2
HD = 128
SH = 48
SP = 64
STATE = 256
CONV = 4
SPAN = 128
SEQ = 1024
MATS = 4
OWNERS = 4
STEP = 4
LANES = 128

highest = lax.Precision.HIGHEST
norm_eps = 1e-05
beta_one = 0.5
beta_two = 0.6
learn_rate = 0.02
adam_eps = 1e-08
weight_decay = 0.1
masked_score = -1e30
NN = ((1,), (0,))
NT = ((1,), (1,))
TN = ((0,), (0,))
bf16 = jnp.bfloat16
f32 = jnp.float32


def mm(left, right, dims, precision=None):
    return lax.dot_general(
        left, right, (dims, ((), ())), preferred_element_type=f32, precision=precision
    )


def silu_value(values):
    return values * jax.nn.sigmoid(values)


def silu_slope(values):
    sigmoid = jax.nn.sigmoid(values)
    return sigmoid * (1.0 + values * (1.0 - sigmoid))


def adam_step(gradient, moment, second, weight):
    moment_new = beta_one * moment + (1.0 - beta_one) * gradient
    second_new = beta_two * second + (1.0 - beta_two) * gradient * gradient
    first_hat = moment_new / (1.0 - beta_one**STEP)
    second_hat = second_new / (1.0 - beta_two**STEP)
    update = -learn_rate * (first_hat / (jnp.sqrt(second_hat) + adam_eps) + weight_decay * weight)
    return (moment_new, second_new, update)


def head_table(heads):
    rows = lax.broadcasted_iota(jnp.int32, (8, heads * SP), 0)
    cols = lax.broadcasted_iota(jnp.int32, (8, heads * SP), 1)
    return (cols // SP == rows).astype(f32)


def head_table_t(heads):
    rows = lax.broadcasted_iota(jnp.int32, (heads * SP, 8), 0)
    cols = lax.broadcasted_iota(jnp.int32, (heads * SP, 8), 1)
    return (rows // SP == cols).astype(f32)


def block_rows(block):
    return pl.ds(pl.multiple_of(block * SPAN, SPAN), SPAN)


def decay_parts(block, a_ref, at_ref, dt_ref, meta_ref, segc_ref, segr_ref, table):
    rows = block_rows(block)
    t_pos = lax.broadcasted_iota(jnp.int32, (SPAN, SPAN), 0)
    s_pos = lax.broadcasted_iota(jnp.int32, (SPAN, SPAN), 1)
    lower = t_pos >= s_pos
    upper = (t_pos <= s_pos).astype(f32)
    run = mm(lower.astype(f32), a_ref[rows, :], NN, highest)
    run_t = mm(at_ref[:, rows], upper, NN, highest)
    live = (segc_ref[rows, :] == segr_ref[:, rows]) & lower
    meta = meta_ref[rows, :]
    same_prev, same_last = meta[:, 0:1], meta[:, 1:2]
    run_last = run[SPAN - 1 : SPAN, :]
    enter = jnp.exp(run) * same_prev
    leave = jnp.exp(run_last - run) * same_last
    passing = jnp.exp(run_last) * same_prev[SPAN - 1 : SPAN, :]
    wide = mm(jnp.concatenate([dt_ref[rows, :], enter, leave], 0), table, NN, highest)
    return rows, run, run_t, live, passing, wide[:SPAN], wide[SPAN : 2 * SPAN], wide[2 * SPAN :]


def decay_of(run, run_t, live, head):
    logs = run[:, head : head + 1] - run_t[head : head + 1, :]
    return jnp.where(live, jnp.exp(jnp.where(live, logs, 0.0)), 0.0)


def mixer_forward_kernel(
    heads, q_heads, q_ref, k_ref, v_ref, xs_ref, z_ref, bm_ref, cm_ref, dt_ref, a_ref, at_ref,
    meta_ref, segc_ref, segr_ref, skip_ref, mix_ref, y_ref, st_ref, state,
):
    q_width = q_heads * HD
    tokens = xs_ref.shape[0]
    table = head_table(heads)
    table_t = head_table_t(heads)
    state[...] = jnp.zeros_like(state)

    def one(block, carry):
        rows, run, run_t, live, passing, dt_w, enter_w, leave_w = decay_parts(
            block, a_ref, at_ref, dt_ref, meta_ref, segc_ref, segr_ref, table
        )
        b_blk, c_blk = bm_ref[rows, :], cm_ref[rows, :]
        x_blk = xs_ref[rows, :].astype(f32)
        inflow = dt_w * x_blk
        inflow_b = inflow.astype(bf16)
        old = state[...]
        st_ref[block] = old
        inter = mm(c_blk, b_blk, NT)
        y_in = enter_w * mm(c_blk, old.astype(bf16), NT)
        parts = []
        for head in range(heads):
            table_h = (decay_of(run, run_t, live, head) * inter).astype(bf16)
            parts.append(mm(table_h, inflow_b[:, head * SP : (head + 1) * SP], NN))
        y_blk = jnp.concatenate(parts, 1) + y_in + skip_ref[...] * x_blk
        y_ref[rows, :] = y_blk
        mix_ref[rows, q_width:] = (y_blk * silu_value(z_ref[rows, :])).astype(bf16)
        pass_col = jnp.sum(table_t * passing, 1, keepdims=True)
        state[...] = pass_col * old + mm((leave_w * inflow).astype(bf16), b_blk, TN)
        return carry

    lax.fori_loop(0, tokens // SPAN, one, 0)
    chunk = 256
    for first in range(0, tokens, chunk):
        known = first + chunk
        rows = slice(first, known)
        q_pos = first + lax.broadcasted_iota(jnp.int32, (chunk, known), 0)
        k_pos = lax.broadcasted_iota(jnp.int32, (chunk, known), 1)
        allowed = (k_pos <= q_pos) & (segc_ref[rows, :] == segr_ref[:, :known])
        for head in range(q_heads):
            lanes = slice(head * HD, (head + 1) * HD)
            scores = mm(q_ref[rows, lanes], k_ref[:known, :], NT) * HD ** (-0.5)
            scores = jnp.where(allowed, scores, masked_score)
            expo = jnp.exp(scores - jnp.max(scores, 1, keepdims=True))
            probs = (expo / jnp.sum(expo, 1, keepdims=True)).astype(bf16)
            mix_ref[rows, lanes] = mm(probs, v_ref[:known, :], NN).astype(bf16)


def mixer_backward_kernel(
    heads, q_heads, gm_ref, q_ref, k_ref, v_ref, xs_ref, z_ref, y_ref, bm_ref, cm_ref, dt_ref,
    a_ref, at_ref, meta_ref, segc_ref, segr_ref, skip_ref, rate_ref, st_ref,
    gq_ref, gk_ref, gv_ref, gz_ref, gx_ref, gdt_ref, gb_ref, gc_ref, small_ref, gskip_ref,
    grad_state,
):
    q_width = q_heads * HD
    tokens = xs_ref.shape[0]
    blocks = tokens // SPAN
    table = head_table(heads)
    table_t = head_table_t(heads)
    grad_state[...] = jnp.zeros_like(grad_state)
    small_ref[...] = jnp.zeros_like(small_ref)
    gskip_ref[...] = jnp.zeros_like(gskip_ref)
    t_pos = lax.broadcasted_iota(jnp.int32, (SPAN, SPAN), 0)
    s_pos = lax.broadcasted_iota(jnp.int32, (SPAN, SPAN), 1)
    upper = (t_pos <= s_pos).astype(f32)

    def one(step, carry):
        block = blocks - 1 - step
        rows, run, run_t, live, passing, dt_w, enter_w, leave_w = decay_parts(
            block, a_ref, at_ref, dt_ref, meta_ref, segc_ref, segr_ref, table
        )
        b_blk, c_blk = bm_ref[rows, :], cm_ref[rows, :]
        x_blk = xs_ref[rows, :].astype(f32)
        z_blk = z_ref[rows, :]
        grad_gated = gm_ref[rows, q_width:].astype(bf16).astype(f32)
        gy = grad_gated * silu_value(z_blk)
        gz_ref[rows, :] = grad_gated * y_ref[rows, :] * silu_slope(z_blk)
        gy_b = gy.astype(bf16)
        inflow = dt_w * x_blk
        inflow_b = inflow.astype(bf16)
        old = st_ref[block]
        old_b = old.astype(bf16)
        later = grad_state[...]
        later_b = later.astype(bf16)
        enter_gy = (enter_w * gy).astype(bf16)
        leave_in = (leave_w * inflow).astype(bf16)
        from_later = leave_w * mm(b_blk, later_b, NT)
        y_in = enter_w * mm(c_blk, old_b, NT)
        inter = mm(c_blk, b_blk, NT)
        grad_inter = jnp.zeros((SPAN, SPAN), f32)
        parts, row_sums, col_sums = [], [], []
        for head in range(heads):
            lanes = slice(head * SP, (head + 1) * SP)
            decay = decay_of(run, run_t, live, head)
            weight = decay * inter
            cross = mm(gy_b[:, lanes], inflow_b[:, lanes], NT)
            grad_inter = grad_inter + decay * cross
            pairs = weight * cross
            row_sums.append(jnp.sum(pairs, 1, keepdims=True))
            col_sums.append(jnp.sum(pairs, 0, keepdims=True))
            parts.append(mm(weight.astype(bf16), gy_b[:, lanes], TN))
        pad = 8 - heads
        row_sum = jnp.concatenate(row_sums + [jnp.zeros((SPAN, pad), f32)], 1)
        col_sum = jnp.concatenate(col_sums + [jnp.zeros((pad, SPAN), f32)], 0)
        grad_inflow = jnp.concatenate(parts, 1) + from_later
        stacked = jnp.concatenate([gy * y_in, inflow * from_later, grad_inflow * x_blk], 0)
        sums = mm(stacked, table_t, NN, highest)
        row_in, col_in, dt_in = sums[:SPAN], sums[SPAN : 2 * SPAN], sums[2 * SPAN :]
        state_dot = jnp.sum(later * old, 1, keepdims=True)
        state_heads = jnp.sum(table_t * state_dot, 0, keepdims=True)
        tail = passing * state_heads + jnp.sum(col_in, 0, keepdims=True)
        grad_a = (
            mm(upper, row_sum + row_in - col_in, NN, highest)
            - mm(upper, col_sum, NT, highest)
            + tail
        )
        dt_blk = dt_ref[rows, :]
        grad_raw = (grad_a * rate_ref[...] + dt_in) * (1.0 - jnp.exp(-dt_blk))
        gdt_ref[rows, :] = grad_raw
        small_ref[0:1, :] += jnp.sum(grad_a * dt_blk, 0, keepdims=True)
        small_ref[1:2, :] += jnp.sum(grad_raw, 0, keepdims=True)
        gskip_ref[...] += jnp.sum(gy * x_blk, 0, keepdims=True)
        gx_ref[rows, :] = grad_inflow * dt_w + skip_ref[...] * gy
        grad_inter_b = grad_inter.astype(bf16)
        gc_ref[rows, :] = (mm(enter_gy, old_b, NN) + mm(grad_inter_b, b_blk, NN)).astype(bf16)
        gb_ref[rows, :] = (mm(leave_in, later_b, NN) + mm(grad_inter_b, c_blk, TN)).astype(bf16)
        pass_col = jnp.sum(table_t * passing, 1, keepdims=True)
        grad_state[...] = pass_col * later + mm(enter_gy, c_blk, TN)
        return carry

    lax.fori_loop(0, blocks, one, 0)
    chunk = 256
    scale = HD ** (-0.5)
    gk_ref[...] = jnp.zeros_like(gk_ref)
    gv_ref[...] = jnp.zeros_like(gv_ref)
    for first in range(0, tokens, chunk):
        known = first + chunk
        rows = slice(first, known)
        q_pos = first + lax.broadcasted_iota(jnp.int32, (chunk, known), 0)
        k_pos = lax.broadcasted_iota(jnp.int32, (chunk, known), 1)
        allowed = (k_pos <= q_pos) & (segc_ref[rows, :] == segr_ref[:, :known])
        for head in range(q_heads):
            lanes = slice(head * HD, (head + 1) * HD)
            q_blk = q_ref[rows, lanes]
            grad_att = gm_ref[rows, lanes].astype(bf16)
            scores = mm(q_blk, k_ref[:known, :], NT) * scale
            scores = jnp.where(allowed, scores, masked_score)
            expo = jnp.exp(scores - jnp.max(scores, 1, keepdims=True))
            probs = expo / jnp.sum(expo, 1, keepdims=True)
            grad_probs = mm(grad_att, v_ref[:known, :], NT)
            gv_ref[:known, :] += mm(probs.astype(bf16), grad_att, TN)
            row_dot = jnp.sum(probs * grad_probs, 1, keepdims=True)
            grad_scores = (probs * (grad_probs - row_dot)).astype(bf16)
            gq_ref[rows, lanes] = mm(grad_scores, k_ref[:known, :], NN) * scale
            gk_ref[:known, :] += mm(grad_scores, q_blk, TN) * scale


def vmem_call(body, out_shape, scratch, name, flops, args):
    size = lambda a: a.size * a.dtype.itemsize
    moved = sum(size(a) for a in args) + sum(size(o) for o in out_shape)
    return pl.pallas_call(
        body,
        out_shape=tuple(out_shape),
        in_specs=[pl.BlockSpec(memory_space=pltpu.VMEM)] * len(args),
        out_specs=tuple([pl.BlockSpec(memory_space=pltpu.VMEM)] * len(out_shape)),
        scratch_shapes=scratch,
        name=name,
        compiler_params=pltpu.CompilerParams(vmem_limit_bytes=60 * 1024 * 1024),
        cost_estimate=pl.CostEstimate(flops=flops, bytes_accessed=moved, transcendentals=0),
    )(*args)


def ring_place():
    n = lax.axis_size("col")
    me = lax.axis_index("col")
    return n, me, lax.rem(me + 1, n), lax.rem(me + n - 1, n), lax.axis_index("row")


def meet(right, left, sibling):
    barrier = pltpu.get_barrier_semaphore()
    for place in ({"col": left}, {"col": right}, {"row": sibling}):
        pl.semaphore_signal(barrier, inc=1, device_id=place, device_id_type=pl.DeviceIdType.MESH)
    pl.semaphore_wait(barrier, 3)


def remote(source, target, send_sem, recv_sem, place):
    return pltpu.make_async_remote_copy(
        src_ref=source,
        dst_ref=target,
        send_sem=send_sem,
        recv_sem=recv_sem,
        device_id=place,
        device_id_type=pl.DeviceIdType.MESH,
    )


def gather_product_kernel(
    pieces, transpose, parts, shard_ref, w_ref, whole_ref, out_ref,
    x_all, w_mine, w_theirs, total, outgoing, incoming,
    ring_send, ring_recv, swap_send, swap_recv, load_sem, own_sem, save_sem, out_sem,
):
    n, me, right, left, row = ring_place()
    sibling = 1 - row
    count = shard_ref.shape[0]
    small = count // parts

    def weight_copies(held, which, base):
        copies, at = [], 0
        for index, (start, stride, size) in enumerate(pieces):
            first = pl.ds(pl.multiple_of(start + stride * which, 16), size)
            spot = pl.ds(at, size)
            if transpose:
                source, target = w_ref.at[first, :], held.at[spot, :]
            else:
                first = pl.ds(pl.multiple_of(start + stride * which, LANES), size)
                source, target = w_ref.at[:, first], held.at[:, spot]
            copies.append(pltpu.make_async_copy(source, target, load_sem.at[base + index]))
            at += size
        return copies

    loads = weight_copies(w_theirs, sibling, 0) + weight_copies(w_mine, row, len(pieces))
    own_rows = pl.ds(pl.multiple_of(me * count, count), count)
    own = pltpu.make_async_copy(shard_ref, x_all.at[own_rows, :], own_sem)
    own.start()
    for copy in loads:
        copy.start()
    meet(right, left, sibling)
    own.wait()

    def owner_of(step):
        return lax.rem(me - step + n, n)

    def ring(step, part):
        rows = pl.ds(pl.multiple_of(owner_of(step) * count + part * small, small), small)
        return remote(
            x_all.at[rows, :], x_all.at[rows, :], ring_send.at[step, part],
            ring_recv.at[step, part], {"col": right},
        )

    def rows_of(step):
        return pl.ds(pl.multiple_of(owner_of(step) * count, count), count)

    def swap(step):
        rows = rows_of(step)
        return remote(
            outgoing.at[rows, :], incoming.at[rows, :], swap_send.at[step], swap_recv.at[step],
            {"row": sibling},
        )

    def finish(step):
        rows = rows_of(step)
        swap(step).wait_recv()
        total[rows, :] = total[rows, :] + incoming[rows, :].astype(f32)
        pltpu.make_async_copy(total.at[rows, :], out_ref.at[rows, :], out_sem.at[step]).start()

    dims = NT if transpose else NN
    for part in range(parts):
        ring(0, part).start()
    for copy in loads:
        copy.wait()

    def one(step, carry):
        for part in range(parts):
            @pl.when(step > 0)
            def _():
                ring(step - 1, part).wait_recv()

            @pl.when((step > 0) & (step < n - 1))
            def _():
                ring(step, part).start()

        rows = rows_of(step)
        block = x_all[rows, :]
        outgoing[rows, :] = mm(block, w_theirs[...], dims).astype(outgoing.dtype)
        swap(step).start()
        total[rows, :] = mm(block, w_mine[...], dims)

        @pl.when(step > 0)
        def _():
            finish(step - 1)

        return carry

    lax.fori_loop(0, n, one, 0)
    save = pltpu.make_async_copy(x_all, whole_ref, save_sem)
    save.start()
    finish(n - 1)
    for step in range(n):
        rows = rows_of(step)
        pltpu.make_async_copy(total.at[rows, :], out_ref.at[rows, :], out_sem.at[step]).wait()
        swap(step).wait_send()
        if step < n - 1:
            for part in range(parts):
                ring(step, part).wait_send()
    save.wait()


def gather_product(shard, weight, pieces, transpose, ident):
    n = lax.axis_size("col")
    count, depth = shard.shape
    tokens = n * count
    width = sum(piece[2] for piece in pieces)
    parts = 2
    w_shape = (width, depth) if transpose else (depth, width)
    flops = 4 * tokens * depth * width
    return pl.pallas_call(
        functools.partial(gather_product_kernel, tuple(pieces), transpose, parts),
        out_shape=(
            jax.ShapeDtypeStruct((tokens, depth), bf16),
            jax.ShapeDtypeStruct((tokens, width), f32),
        ),
        in_specs=[pl.BlockSpec(memory_space=pl.ANY)] * 2,
        out_specs=(pl.BlockSpec(memory_space=pl.ANY), pl.BlockSpec(memory_space=pl.ANY)),
        scratch_shapes=[
            pltpu.VMEM((tokens, depth), bf16),
            pltpu.VMEM(w_shape, bf16),
            pltpu.VMEM(w_shape, bf16),
            pltpu.VMEM((tokens, width), f32),
            pltpu.VMEM((tokens, width), bf16),
            pltpu.VMEM((tokens, width), bf16),
            pltpu.SemaphoreType.DMA((n, parts)),
            pltpu.SemaphoreType.DMA((n, parts)),
            pltpu.SemaphoreType.DMA((n,)),
            pltpu.SemaphoreType.DMA((n,)),
            pltpu.SemaphoreType.DMA((2 * len(pieces),)),
            pltpu.SemaphoreType.DMA,
            pltpu.SemaphoreType.DMA,
            pltpu.SemaphoreType.DMA((n,)),
        ],
        name="gather_product_%d" % ident,
        compiler_params=pltpu.CompilerParams(
            collective_id=ident, has_side_effects=True, vmem_limit_bytes=40 * 1024 * 1024
        ),
        cost_estimate=pl.CostEstimate(
            flops=flops, bytes_accessed=6 * tokens * width + 120_000_000, transcendentals=0
        ),
    )(shard, weight)


def product_scatter_kernel(
    pieces, common, transpose, parts, *refs
):
    own_ref, refs = refs[0], refs[1:]
    both_ref = None
    if common:
        both_ref, refs = refs[0], refs[1:]
    (w_ref, whole_ref, out_ref, h_all, w_all, sums, outgoing, incoming, final,
     ring_send, ring_recv, swap_send, swap_recv, own_sem, both_sem, load_sem, save_sem, out_sem) = refs
    n, me, right, left, row = ring_place()
    sibling = 1 - row
    tokens = own_ref.shape[0]
    count = tokens // n
    small = count // parts

    def rows_of(step):
        chunk = lax.rem(me - 1 - step + 2 * n, n)
        return pl.ds(pl.multiple_of(chunk * count, count), count)

    def columns(which):
        spots, at = [], 0
        for start, stride, size in pieces:
            spots.append((pl.ds(at, size), pl.ds(pl.multiple_of(start + stride * which, LANES), size)))
            at += size
        return spots

    load = pltpu.make_async_copy(w_ref, w_all, load_sem)
    load.start()

    def own_copies(step):
        rows = rows_of(step)
        return [
            pltpu.make_async_copy(own_ref.at[rows, a], h_all.at[rows, b], own_sem.at[step, index])
            for index, (a, b) in enumerate(columns(row))
        ]

    def swaps(step):
        rows = rows_of(step)
        return [
            remote(own_ref.at[rows, a], h_all.at[rows, b], swap_send.at[step, index],
                   swap_recv.at[step, index], {"row": sibling})
            for index, (a, b) in enumerate(columns(row))
        ]

    def both_copy(step):
        rows = rows_of(step)
        return pltpu.make_async_copy(
            both_ref.at[rows, :], h_all.at[rows, pl.ds(common[0], common[1])], both_sem.at[step]
        )

    for step in range(n):
        for copy in own_copies(step):
            copy.start()
        if common:
            both_copy(step).start()
    meet(right, left, sibling)
    for step in range(n):
        for copy in swaps(step):
            copy.start()
    load.wait()
    dims = NT if transpose else NN

    def ring(step, part):
        rows = pl.ds(part * small, small)
        return remote(
            outgoing.at[step, rows, :], incoming.at[step, rows, :], ring_send.at[step, part],
            ring_recv.at[step, part], {"col": right},
        )

    def one(step, carry):
        rows = rows_of(step)
        for copy in own_copies(step):
            copy.wait()
        if common:
            both_copy(step).wait()
        for copy in swaps(step):
            copy.wait_recv()
        sums[...] = mm(h_all[rows, :], w_all[...], dims)
        for part in range(parts):
            some = pl.ds(part * small, small)

            @pl.when(step > 0)
            def _():
                ring(step - 1, part).wait_recv()
                sums[some, :] = sums[some, :] + incoming[step - 1, some, :].astype(f32)

            @pl.when(step < n - 1)
            def _():
                outgoing[step, some, :] = sums[some, :].astype(bf16)
                ring(step, part).start()

        return carry

    lax.fori_loop(0, n, one, 0)
    out = pltpu.make_async_copy(sums, out_ref, out_sem)
    out.start()
    save = pltpu.make_async_copy(h_all, whole_ref, save_sem)
    save.start()
    for step in range(n):
        for copy in swaps(step):
            copy.wait_send()
        if step < n - 1:
            for part in range(parts):
                ring(step, part).wait_send()
    out.wait()
    save.wait()


def product_scatter(own, weight, pieces, common, both, transpose, ident):
    n = lax.axis_size("col")
    tokens = own.shape[0]
    count = tokens // n
    depth, width = weight.shape[::-1] if transpose else weight.shape
    parts = 2
    operands = (own, both, weight) if common else (own, weight)
    return pl.pallas_call(
        functools.partial(product_scatter_kernel, tuple(pieces), common, transpose, parts),
        out_shape=(
            jax.ShapeDtypeStruct((tokens, depth), bf16),
            jax.ShapeDtypeStruct((count, width), f32),
        ),
        in_specs=[pl.BlockSpec(memory_space=pl.ANY)] * len(operands),
        out_specs=(pl.BlockSpec(memory_space=pl.ANY), pl.BlockSpec(memory_space=pl.ANY)),
        scratch_shapes=[
            pltpu.VMEM((tokens, depth), bf16),
            pltpu.VMEM(weight.shape, bf16),
            pltpu.VMEM((count, width), f32),
            pltpu.VMEM((n - 1, count, width), bf16),
            pltpu.VMEM((n - 1, count, width), bf16),
            pltpu.VMEM((8, LANES), f32),
            pltpu.SemaphoreType.DMA((n, parts)),
            pltpu.SemaphoreType.DMA((n, parts)),
            pltpu.SemaphoreType.DMA((n, len(pieces))),
            pltpu.SemaphoreType.DMA((n, len(pieces))),
            pltpu.SemaphoreType.DMA((n, len(pieces))),
            pltpu.SemaphoreType.DMA((n,)),
            pltpu.SemaphoreType.DMA,
            pltpu.SemaphoreType.DMA,
            pltpu.SemaphoreType.DMA,
        ],
        name="product_scatter_%d" % ident,
        compiler_params=pltpu.CompilerParams(
            collective_id=ident, has_side_effects=True, vmem_limit_bytes=40 * 1024 * 1024
        ),
        cost_estimate=pl.CostEstimate(
            flops=2 * tokens * depth * width, bytes_accessed=130_000_000, transcendentals=0
        ),
    )(*operands)


def shares_kernel(quarters, spans, held_ref, m_ref, v_ref, out_ref, zeros, taken, given, in_sem, out_sem, zero_sem):
    n = out_ref.shape[0]
    slot_rows = m_ref.shape[0] // 2
    zeros[...] = jnp.zeros_like(zeros)
    plan, at = [], 0
    for index, rows in enumerate(quarters):
        for source in (m_ref, v_ref):
            plan.append((index, rows, source, at))
            at += spans[index]
    for item, (index, rows, source, at) in enumerate(plan):
        blanks = [
            pltpu.make_async_copy(
                zeros.at[pl.ds(0, rows), :], out_ref.at[d, pl.ds(at, rows), :], zero_sem.at[item, d]
            )
            for d in range(n)
        ]

        @pl.when(held_ref[index] < 0)
        def _():
            for copy in blanks:
                copy.start()

    for item, (index, rows, source, at) in enumerate(plan):

        @pl.when(held_ref[index] >= 0)
        def _():
            base = held_ref[index] * slot_rows

            def fetch(d):
                first = pl.multiple_of(base + d * rows, 8)
                return pltpu.make_async_copy(
                    source.at[pl.ds(first, rows), :], taken.at[d % 2, pl.ds(0, rows), :],
                    in_sem.at[d % 2],
                )

            def store(d):
                return pltpu.make_async_copy(
                    given.at[d % 2, pl.ds(0, rows), :], out_ref.at[d, pl.ds(at, rows), :],
                    out_sem.at[d % 2],
                )

            fetch(0).start()
            for d in range(n):
                if d + 1 < n:
                    fetch(d + 1).start()
                fetch(d).wait()
                if d >= 2:
                    store(d - 2).wait()
                given[d % 2, pl.ds(0, rows), :] = taken[d % 2, pl.ds(0, rows), :].astype(bf16)
                store(d).start()
            for d in range(max(n - 2, 0), n):
                store(d).wait()

    for item, (index, rows, source, at) in enumerate(plan):
        blanks = [
            pltpu.make_async_copy(
                zeros.at[pl.ds(0, rows), :], out_ref.at[d, pl.ds(at, rows), :], zero_sem.at[item, d]
            )
            for d in range(n)
        ]

        @pl.when(held_ref[index] < 0)
        def _():
            for copy in blanks:
                copy.wait()


def moment_shares(held, moments, seconds, quarters, spans, n):
    largest = max(quarters)
    any_spec = pl.BlockSpec(memory_space=pl.ANY)
    total = 2 * sum(spans)
    return pl.pallas_call(
        functools.partial(shares_kernel, tuple(quarters), tuple(spans)),
        out_shape=jax.ShapeDtypeStruct((n, total, LANES), bf16),
        in_specs=[pl.BlockSpec(memory_space=pltpu.SMEM), any_spec, any_spec],
        out_specs=any_spec,
        scratch_shapes=[
            pltpu.VMEM((largest, LANES), bf16),
            pltpu.VMEM((2, largest, LANES), f32),
            pltpu.VMEM((2, largest, LANES), bf16),
            pltpu.SemaphoreType.DMA((2,)),
            pltpu.SemaphoreType.DMA((2,)),
            pltpu.SemaphoreType.DMA((2 * len(quarters), n)),
        ],
        name="moment_shares",
        cost_estimate=pl.CostEstimate(flops=0, bytes_accessed=45_000_000, transcendentals=0),
    )(held, moments, seconds)


def fresh_weight(grad, moment, second, weight):
    weight = weight.astype(f32)
    update = adam_step(grad.astype(f32), moment.astype(f32), second.astype(f32), weight)[2]
    return (weight + update).astype(bf16)


def share_step_kernel(g_ref, m_ref, v_ref, w_ref, out_ref):
    out_ref[...] = fresh_weight(g_ref[...], m_ref[...], v_ref[...], w_ref[...])


def share_step(grad, moment, second, weight):
    rows = grad.shape[0]
    block = min(rows, 1024)
    spec = pl.BlockSpec((block, LANES), lambda j: (j, 0))
    return pl.pallas_call(
        share_step_kernel,
        grid=(pl.cdiv(rows, block),),
        out_shape=jax.ShapeDtypeStruct((rows, LANES), bf16),
        in_specs=[spec] * 4,
        out_specs=spec,
        name="share_step",
        cost_estimate=pl.CostEstimate(
            flops=10 * grad.size, bytes_accessed=10 * grad.size, transcendentals=grad.size
        ),
    )(grad, moment, second, weight)


UNIT = 1648


def settle_kernel(held_ref, got_ref, m_ref, v_ref, w_ref, out_ref):
    @pl.when(held_ref[0] >= 0)
    def _():
        out_ref[...] = fresh_weight(
            got_ref[...], m_ref[...].astype(bf16), v_ref[...].astype(bf16), w_ref[...]
        )

    @pl.when(held_ref[0] < 0)
    def _():
        out_ref[...] = got_ref[...]


def settle(held, got, moments, seconds, weight):
    rows = got.shape[0]
    slot_blocks = moments.shape[0] // 2 // UNIT

    def state_at(j, held_ref):
        return (jnp.where(held_ref[0] >= 0, held_ref[0] * slot_blocks + j, 0), 0)

    def weight_at(j, held_ref):
        return (jnp.where(held_ref[0] >= 0, j, 0), 0)

    plain = pl.BlockSpec((UNIT, LANES), lambda j, held_ref: (j, 0))
    return pl.pallas_call(
        settle_kernel,
        grid_spec=pltpu.PrefetchScalarGridSpec(
            num_scalar_prefetch=1,
            grid=(pl.cdiv(rows, UNIT),),
            in_specs=[
                plain,
                pl.BlockSpec((UNIT, LANES), state_at),
                pl.BlockSpec((UNIT, LANES), state_at),
                pl.BlockSpec((UNIT, LANES), weight_at),
            ],
            out_specs=plain,
        ),
        out_shape=jax.ShapeDtypeStruct((rows, LANES), bf16),
        name="settle",
        cost_estimate=pl.CostEstimate(
            flops=10 * got.size, bytes_accessed=12 * got.size, transcendentals=got.size
        ),
    )(held, got, moments, seconds, weight)


def owner_kernel(sizes, which_ref, block_ref, m_ref, v_ref, *refs):
    g_refs, w_refs = refs[:MATS], refs[MATS : 2 * MATS]
    grad_ref, m_out, v_out, u_out = refs[2 * MATS :]
    step = pl.program_id(0)
    which = which_ref[step]
    rows = block_ref[step] * UNIT + lax.broadcasted_iota(jnp.int32, (UNIT, LANES), 0)

    @pl.when(which < 0)
    def _():
        for out in (grad_ref, m_out, v_out, u_out):
            out[...] = jnp.zeros_like(out)

    for index in range(MATS):

        @pl.when(which == index)
        def _():
            inside = rows < sizes[index]
            grad = jnp.where(inside, g_refs[index][...].astype(f32), 0.0)
            weight = jnp.where(inside, w_refs[index][...].astype(f32), 0.0)
            grad_ref[...] = grad
            m_out[...], v_out[...], u_out[...] = adam_step(grad, m_ref[...], v_ref[...], weight)


def owner_outputs(which, block, moments, seconds, grads, weights):
    rows = moments.shape[0]
    sizes = tuple(g.shape[0] for g in grads)

    def chosen(index):
        last = pl.cdiv(sizes[index], UNIT) - 1

        def at(j, which_ref, block_ref):
            return (jnp.where(which_ref[j] == index, jnp.minimum(block_ref[j], last), 0), 0)

        return pl.BlockSpec((UNIT, LANES), at)

    plain = pl.BlockSpec((UNIT, LANES), lambda j, which_ref, block_ref: (j, 0))
    picks = [chosen(index) for index in range(MATS)]
    return pl.pallas_call(
        functools.partial(owner_kernel, sizes),
        grid_spec=pltpu.PrefetchScalarGridSpec(
            num_scalar_prefetch=2,
            grid=(rows // UNIT,),
            in_specs=[plain, plain] + picks + picks,
            out_specs=[plain] * 4,
        ),
        out_shape=[jax.ShapeDtypeStruct((rows, LANES), f32)] * 4,
        name="owner_outputs",
        cost_estimate=pl.CostEstimate(
            flops=12 * rows * LANES, bytes_accessed=26 * rows * LANES, transcendentals=rows * LANES
        ),
    )(which, block, moments, seconds, *grads, *weights)


def row_total(values):
    return lax.psum(values, "row")


def conv_shift(values, segments, lag):
    if lag == 0:
        return values
    tokens = values.shape[0]
    pad = jnp.zeros((abs(lag), values.shape[1]), values.dtype)
    foreign = jnp.full((abs(lag),), -1, jnp.int32)
    if lag > 0:
        moved = jnp.concatenate([pad, values[: tokens - lag]], 0)
        other = jnp.concatenate([foreign, segments[: tokens - lag]], 0)
    else:
        moved = jnp.concatenate([values[-lag:], pad], 0)
        other = jnp.concatenate([segments[-lag:], foreign], 0)
    return jnp.where((other == segments)[:, None], moved, 0.0)


def norm_back(grad_act, normed, scale_rows, gain):
    weighted = grad_act * gain
    inner_sum = row_total(jnp.sum(weighted * normed, 1))
    grad_in = scale_rows[:, None] * (weighted - normed * (inner_sum / D)[:, None])
    return (grad_in, jnp.sum(grad_act * normed, 0))


def shards(
    x_in,
    cotangent,
    segment_ids,
    owner,
    w_mix_in,
    w_mix_out,
    w_gate_up,
    w_down,
    mat_m,
    mat_v,
    small_params,
    small_m,
    small_v,
):
    n_row = lax.axis_size("row")
    n_col = lax.axis_size("col")
    n_dp = lax.axis_size("dp")
    row_index = lax.axis_index("row")
    col_index = lax.axis_index("col")
    dp_index = lax.axis_index("dp")
    tokens = SEQ
    width_row = x_in.shape[1]
    q_width = QH * HD // n_col
    sub = STATE // n_col
    shared_width = 4 * sub
    ssm_width = SH * SP // n_col
    head_count = SH // n_col
    ff_width = FF // n_col
    mix_width = q_width + ssm_width
    conv_width = SH * SP + 2 * STATE
    col_z = q_width + shared_width
    col_x = col_z + ssm_width
    col_dt = col_x + ssm_width
    q_own = q_width // n_row
    ssm_own = ssm_width // n_row
    heads = head_count // n_row
    q_heads = q_own // HD
    ff_own = ff_width // n_row
    at_kv = q_own
    at_z = at_kv + shared_width
    at_x = at_z + ssm_own
    at_dt = at_x + ssm_own
    segs = segment_ids[0]

    off_alog = 2 * D
    off_dtb = 2 * D + SH
    off_skip = 2 * D + 2 * SH
    off_kern = 2 * D + 3 * SH
    off_cbias = off_kern + CONV * conv_width
    first_head = col_index * head_count + row_index * heads
    gain_one = lax.dynamic_slice_in_dim(small_params, row_index * width_row, width_row)
    gain_two = lax.dynamic_slice_in_dim(small_params, D + row_index * width_row, width_row)

    def own_heads(offset):
        return lax.dynamic_slice_in_dim(small_params, offset + first_head, heads)

    a_log_own, dt_bias_own, skip_own = own_heads(off_alog), own_heads(off_dtb), own_heads(off_skip)
    conv_table = small_params[off_kern:].reshape(CONV + 1, conv_width)

    def own_channels(table):
        return jnp.concatenate(
            [
                lax.dynamic_slice_in_dim(table, SH * SP + col_index * sub, sub, 1),
                lax.dynamic_slice_in_dim(table, SH * SP + STATE + col_index * sub, sub, 1),
                lax.dynamic_slice_in_dim(table, first_head * SP, ssm_own, 1),
            ],
            1,
        )

    conv_own = own_channels(conv_table)
    kern_own, bias_own = conv_own[:CONV], conv_own[CONV]
    rate = -jnp.exp(a_log_own)

    def pad_heads(values):
        return jnp.pad(values, [(0, 0)] * (values.ndim - 1) + [(0, 8 - heads)])

    w_in_t = w_mix_in.T
    dt_rows = w_in_t[col_dt:].reshape(n_row, heads, width_row)
    dt_rows = jnp.pad(dt_rows, ((0, 0), (0, LANES - heads), (0, 0)))

    w_in_full = jnp.concatenate([w_in_t[:col_dt], dt_rows.reshape(n_row * LANES, width_row)], 0)

    xf = x_in.astype(f32)
    scale_one = lax.rsqrt(row_total(jnp.sum(xf * xf, 1)) / D + norm_eps)
    normed_one = xf * scale_one[:, None]
    act_one = (normed_one * gain_one).astype(bf16)
    in_pieces = [
        (0, q_own, q_own),
        (q_width, 0, shared_width),
        (col_z, ssm_own, ssm_own),
        (col_x, ssm_own, ssm_own),
        (col_dt, LANES, LANES),
    ]
    gu_pieces = [(0, ff_own, ff_own), (ff_width, ff_own, ff_own)]
    mix_pieces = [(0, q_own, q_own), (q_width, ssm_own, ssm_own)]
    down_pieces = [(0, ff_own, ff_own)]
    act_one_g, proj = gather_product(act_one, w_in_full, in_pieces, True, 0)

    queries = proj[:, :at_kv].astype(bf16)
    kv_own = proj[:, at_kv : at_kv + 2 * sub]
    z_gate = proj[:, at_z:at_x]
    dt_raw = proj[:, at_dt : at_dt + heads]
    conv_in = jnp.concatenate([proj[:, at_kv + 2 * sub : at_z], proj[:, at_x:at_dt]], 1)
    conv_out = bias_own
    for lag in range(CONV):
        conv_out = conv_out + kern_own[lag] * conv_shift(conv_in, segs, lag)
    bc_pre, x_pre = conv_out[:, : 2 * sub], conv_out[:, 2 * sub :]
    x_sig = silu_value(x_pre).astype(bf16)
    shared = jnp.concatenate([kv_own, silu_value(bc_pre)], 1).astype(bf16)
    half = tokens // n_row
    shared_half = lax.dynamic_slice_in_dim(shared, row_index * half, half)
    features = lax.all_gather(shared_half, ("row", "col"), axis=0)
    features = features.reshape(n_row, n_col, half, 4, sub).transpose(3, 0, 2, 1, 4)
    features = features.reshape(4, tokens, STATE)
    q_local = QH // n_col
    kv_head = col_index * q_local // (QH // KVH)
    key_head = lax.dynamic_slice_in_dim(features[0], kv_head * HD, HD, 1)
    val_head = lax.dynamic_slice_in_dim(features[1], kv_head * HD, HD, 1)
    b_mat, c_mat = features[2], features[3]

    dt = jax.nn.softplus(dt_raw + dt_bias_own)
    dt_pad = pad_heads(dt)
    a_pad = pad_heads(dt * rate)
    seg_blocks = segs.reshape(tokens // SPAN, SPAN)
    before = jnp.concatenate([jnp.full((1,), -1, jnp.int32), seg_blocks[:-1, -1]])
    same_prev = (seg_blocks == before[:, None]).reshape(tokens)
    same_last = (seg_blocks == seg_blocks[:, -1:]).reshape(tokens)
    meta = jnp.stack([same_prev, same_last], 1).astype(f32)
    seg_col, seg_row = segs[:, None], segs[None, :]
    skip_wide = jnp.repeat(skip_own, SP)[None, :]
    common = (dt_pad, a_pad, a_pad.T, meta, seg_col, seg_row, skip_wide)
    n_blocks = tokens // SPAN
    mix_own, y_ssm, states = vmem_call(
        functools.partial(mixer_forward_kernel, heads, q_heads),
        [
            jax.ShapeDtypeStruct((tokens, q_own + ssm_own), bf16),
            jax.ShapeDtypeStruct((tokens, ssm_own), f32),
            jax.ShapeDtypeStruct((n_blocks, ssm_own, STATE), f32),
        ],
        [pltpu.VMEM((ssm_own, STATE), f32)],
        "mixer_forward",
        1_000_000_000,
        (queries, key_head, val_head, x_sig, z_gate, b_mat, c_mat) + common,
    )
    mix_g, mix_sum = product_scatter(mix_own, w_mix_out, mix_pieces, None, None, False, 1)
    hidden_one = xf + mix_sum
    scale_two = lax.rsqrt(row_total(jnp.sum(hidden_one * hidden_one, 1)) / D + norm_eps)
    normed_two = hidden_one * scale_two[:, None]
    act_two = (normed_two * gain_two).astype(bf16)
    act_two_g, gate_up = gather_product(act_two, w_gate_up, gu_pieces, False, 2)
    gate, upper = gate_up[:, :ff_own], gate_up[:, ff_own:]
    inner = (silu_value(gate) * upper).astype(bf16)
    inner_g, down_sum = product_scatter(inner, w_down, down_pieces, None, None, False, 3)
    y_out = (hidden_one + down_sum).astype(bf16)

    grad_out_g, grad_inner = gather_product(cotangent, w_down, down_pieces, True, 4)
    grad_down_w = mm(inner_g, grad_out_g, TN).astype(bf16)
    grad_gu = jnp.concatenate(
        [grad_inner * upper * silu_slope(gate), grad_inner * silu_value(gate)], 1
    ).astype(bf16)
    grad_gu_g, grad_act_two = product_scatter(grad_gu, w_gate_up, gu_pieces, None, None, True, 5)
    grad_gu_w = mm(act_two_g, grad_gu_g, TN).astype(bf16)
    grad_norm_two, gain_two_part = norm_back(grad_act_two, normed_two, scale_two, gain_two)
    grad_hidden = cotangent.astype(f32) + grad_norm_two
    grad_hidden_g, grad_mix = gather_product(
        grad_hidden.astype(bf16), w_mix_out, mix_pieces, True, 6
    )
    grad_mix_w = mm(mix_g, grad_hidden_g, TN).astype(bf16)

    shape = lambda cols, kind: jax.ShapeDtypeStruct((tokens, cols), kind)
    grad_q, grad_k, grad_v, grad_z, grad_x, grad_dt, grad_b, grad_c, small_sums, grad_skip = vmem_call(
        functools.partial(mixer_backward_kernel, heads, q_heads),
        [
            shape(q_own, f32), shape(HD, f32), shape(HD, f32), shape(ssm_own, f32),
            shape(ssm_own, f32), shape(8, f32), shape(STATE, bf16), shape(STATE, bf16),
            jax.ShapeDtypeStruct((8, 8), f32), jax.ShapeDtypeStruct((1, ssm_own), f32),
        ],
        [pltpu.VMEM((ssm_own, STATE), f32)],
        "mixer_backward",
        3_000_000_000,
        (grad_mix, queries, key_head, val_head, x_sig, z_gate, y_ssm, b_mat, c_mat)
        + common
        + (pad_heads(rate)[None, :], states),
    )
    zero_kv = jnp.zeros((tokens, KVH * HD), bf16)
    keys_full = lax.dynamic_update_slice(zero_kv, grad_k.astype(bf16), (0, kv_head * HD))
    vals_full = lax.dynamic_update_slice(zero_kv, grad_v.astype(bf16), (0, kv_head * HD))
    term = jnp.stack([keys_full, vals_full, grad_b, grad_c], 1)
    term = term.reshape(n_row, half, 4, n_col, sub).transpose(0, 3, 1, 2, 4)
    term = term.reshape(n_row * n_col, half, shared_width)
    shared_sum = lax.psum_scatter(term, ("row", "col"), scatter_dimension=0, tiled=False)
    grad_shared = lax.all_gather(shared_sum, "row", axis=0, tiled=True).astype(f32)
    grad_conv = jnp.concatenate(
        [grad_shared[:, 2 * sub :] * silu_slope(bc_pre), grad_x * silu_slope(x_pre)], 1
    ).astype(bf16).astype(f32)
    bias_grad = jnp.sum(grad_conv, 0)
    grad_conv_raw = kern_own[0] * grad_conv
    kern_grad = [jnp.sum(grad_conv * conv_in, 0)]
    for lag in range(1, CONV):
        grad_conv_raw = grad_conv_raw + kern_own[lag] * conv_shift(grad_conv, segs, -lag)
        kern_grad.append(jnp.sum(grad_conv * conv_shift(conv_in, segs, lag), 0))
    kern_grad = jnp.stack(kern_grad)
    raw_own = jnp.concatenate(
        [grad_q, grad_z, grad_conv_raw[:, 2 * sub :], jnp.pad(grad_dt, ((0, 0), (0, LANES - 8)))], 1
    ).astype(bf16)
    raw_kvbc = jnp.concatenate([grad_shared[:, : 2 * sub], grad_conv_raw[:, : 2 * sub]], 1).astype(bf16)
    raw_pieces = [piece for index, piece in enumerate(in_pieces) if index != 1]
    raw_g, grad_act_one = product_scatter(
        raw_own, w_in_full, raw_pieces, (q_width, shared_width), raw_kvbc, False, 7
    )
    in_w = mm(act_one_g, raw_g, TN).astype(bf16)
    grad_in_w = jnp.concatenate(
        [in_w[:, :col_dt]]
        + [in_w[:, col_dt + r * LANES : col_dt + r * LANES + heads] for r in range(n_row)],
        1,
    )
    grad_norm_one, gain_one_part = norm_back(grad_act_one, normed_one, scale_one, gain_one)
    x_grad = (grad_hidden + grad_norm_one).astype(bf16)

    small_own = jnp.concatenate(
        [
            gain_one_part,
            gain_two_part,
            small_sums[0, :heads] * rate,
            small_sums[1, :heads],
            jnp.sum(grad_skip.reshape(heads, SP), 1),
            kern_grad.reshape(-1),
            bias_grad,
        ]
    )
    small_len = small_own.shape[0]
    small_rows = -(-small_len // (8 * LANES)) * 8
    small_own = jnp.pad(small_own, (0, small_rows * LANES - small_len)).reshape(small_rows, LANES)
    everyone = lax.all_gather(small_own, ("dp", "row", "col"), axis=0, tiled=True)
    everyone = everyone.reshape(n_dp, n_row, n_col, small_rows * LANES)
    total = jnp.sum(everyone, 0)[..., :small_len]
    pieces = jnp.split(
        total,
        [
            width_row, 2 * width_row, 2 * width_row + heads, 2 * width_row + 2 * heads,
            2 * width_row + 3 * heads,
        ],
        axis=2,
    )

    def by_head(values):
        return values.transpose(1, 0, 2).reshape(-1)

    conv_sum = pieces[5].reshape(n_row, n_col, CONV + 1, 2 * sub + ssm_own)
    x_sum = conv_sum[..., 2 * sub :].transpose(2, 1, 0, 3).reshape(CONV + 1, SH * SP)
    b_sum = conv_sum[0, ..., :sub].transpose(1, 0, 2).reshape(CONV + 1, STATE)
    c_sum = conv_sum[0, ..., sub : 2 * sub].transpose(1, 0, 2).reshape(CONV + 1, STATE)
    small_grad = jnp.concatenate(
        [
            jnp.sum(pieces[0], 1).reshape(-1),
            jnp.sum(pieces[1], 1).reshape(-1),
            by_head(pieces[2]),
            by_head(pieces[3]),
            by_head(pieces[4]),
            jnp.concatenate([x_sum, b_sum, c_sum], 1).reshape(-1),
        ]
    )
    small_moment, small_second, small_update = adam_step(small_grad, small_m, small_v, small_params)

    weights_local = (w_mix_in, w_mix_out, w_gate_up, w_down)
    grads_local = (grad_in_w, grad_mix_w, grad_gu_w, grad_down_w)
    group_size = n_dp // OWNERS
    piece_len = mat_m.shape[-1]
    my_group = dp_index // group_size
    my_piece = dp_index % group_size
    sizes = [w.size for w in weights_local]
    slot_len = max(sizes)
    moments = mat_m.reshape(piece_len // LANES, LANES)
    seconds = mat_v.reshape(piece_len // LANES, LANES)
    slot_rows = slot_len // LANES
    rows_of = [size // LANES for size in sizes]
    quarters = [rows // n_dp for rows in rows_of]
    spans = [-(-rows // 32) * 32 for rows in quarters]
    ranks = []
    for index in range(MATS):
        earlier = jnp.int32(0)
        for other in range(index):
            earlier = earlier + (owner[other] == owner[index]).astype(jnp.int32)
        ranks.append(earlier)
    held = jnp.stack([jnp.where(owner[i] == my_group, ranks[i], -1) for i in range(MATS)])

    def flat(matrix):
        return matrix.reshape(-1, LANES)

    def own_share(matrix):
        count = matrix.shape[0] // n_dp
        return flat(lax.dynamic_slice_in_dim(matrix, dp_index * count, count))

    def share_sum(values):
        count, width = values.shape[1:]
        values = values.reshape(n_dp * count, width)
        return lax.psum_scatter(values, "dp", scatter_dimension=0, tiled=True)

    def in_shares(values, index):
        values = values.reshape(n_dp, quarters[index], LANES)
        return jnp.pad(values, ((0, 0), (0, spans[index] - quarters[index]), (0, 0)))

    if group_size == 1:
        shares = moment_shares(held, moments, seconds, quarters, spans, n_dp)
    else:
        parts = []
        for index in range(MATS):
            at = ranks[index] * slot_rows - my_piece * moments.shape[0]
            entry = jnp.arange(rows_of[index]) + at
            inside = (held[index] >= 0) & (entry >= 0) & (entry < moments.shape[0])
            for buffer in (moments, seconds):
                wide = jnp.pad(buffer, ((slot_rows, slot_rows), (0, 0)))
                first = jnp.clip(at + slot_rows, 0, moments.shape[0] + slot_rows)
                cut = lax.dynamic_slice_in_dim(wide, first, rows_of[index])
                cut = jnp.where(inside[:, None], cut, 0.0).astype(bf16)
                parts.append(in_shares(cut, index))
        shares = jnp.concatenate(parts, 1)
    shares = share_sum(shares)
    moment_share, second_share, at = [], [], 0
    for rows, span in zip(quarters, spans):
        moment_share.append(shares[at : at + rows])
        second_share.append(shares[at + span : at + span + rows])
        at += 2 * span

    flat_w = [flat(w) for w in weights_local]
    flat_g, new_weights = [None] * MATS, [None] * MATS
    for group in ((3, 2), (1, 0)):
        cut = jnp.concatenate([in_shares(flat(grads_local[i]), i) for i in group], 1)
        cut = share_sum(cut)
        grad_share, fresh_share, at = {}, {}, 0
        for i in group:
            grad_share[i] = cut[at : at + quarters[i]]
            fresh_share[i] = share_step(
                grad_share[i], moment_share[i], second_share[i], own_share(weights_local[i])
            )
            at += spans[i]
        if group_size == 1:
            sent = jnp.concatenate(
                [
                    jnp.where(
                        (owner[i] == jnp.arange(n_dp))[:, None, None],
                        grad_share[i][None],
                        fresh_share[i][None],
                    )
                    for i in group
                ],
                1,
            )
            got = lax.all_to_all(sent, "dp", 0, 0)
            at = 0
            for i in group:
                flat_g[i] = got[:, at : at + quarters[i]].reshape(rows_of[i], LANES)
                fresh = settle(held[i : i + 1], flat_g[i], moments, seconds, flat_w[i])
                new_weights[i] = fresh.reshape(weights_local[i].shape)
                at += quarters[i]
        else:
            both = jnp.concatenate([grad_share[i] for i in group] + [fresh_share[i] for i in group], 0)
            got = lax.all_gather(both, "dp", axis=0)
            at, half_rows = 0, both.shape[0] // 2
            for i in group:
                flat_g[i] = got[:, at : at + quarters[i]].reshape(rows_of[i], LANES)
                fresh = got[:, half_rows + at : half_rows + at + quarters[i]]
                new_weights[i] = fresh.reshape(weights_local[i].shape)
                at += quarters[i]

    first_row = my_piece * moments.shape[0] + jnp.arange(moments.shape[0] // UNIT) * UNIT
    which = jnp.full(first_row.shape, -1, jnp.int32)
    for index in range(MATS):
        which = jnp.where(held[index] == first_row // slot_rows, index, which)
    block = (first_row % slot_rows // UNIT).astype(jnp.int32)
    grad_piece, moment_new, second_new, update = owner_outputs(
        which.astype(jnp.int32), block, moments, seconds, flat_g, flat_w
    )
    out_shape = (1, 1, 1, piece_len)
    return (
        y_out,
        x_grad,
        grad_piece.reshape(out_shape),
        moment_new.reshape(out_shape),
        second_new.reshape(out_shape),
        update.reshape(out_shape),
        new_weights[0],
        new_weights[1],
        new_weights[2],
        new_weights[3],
        small_grad,
        small_moment,
        small_second,
        small_update,
    )


def solution(mesh):
    placed = (
        P(("dp", "col"), "row"),
        P(("dp", "col"), "row"),
        P("dp", None),
        P(),
        P("row", "col"),
        P("col", "row"),
        P("row", "col"),
        P("col", "row"),
        P("row", "col", "dp", None),
        P("row", "col", "dp", None),
        P(),
        P(),
        P(),
    )
    return jax.shard_map(
        shards,
        mesh=mesh,
        in_specs=placed,
        out_specs=(
            P(("dp", "col"), "row"),
            P(("dp", "col"), "row"),
            P("row", "col", "dp", None),
            P("row", "col", "dp", None),
            P("row", "col", "dp", None),
            P("row", "col", "dp", None),
            P("row", "col"),
            P("col", "row"),
            P("row", "col"),
            P("col", "row"),
            P(),
            P(),
            P(),
            P(),
        ),
        check_vma=False,
    )
```
